32 devices in a mesh: dp: 8 (over z, core), tensor: 4 (over y, x).
Axes of the slice: x: 2, y: 2, z: 4, core: 2. Of those that a mesh axis runs over, the one named last changes fastest.
Arguments:
- hidden_in: bfloat16 [8192, 5120], P(('dp', 'tensor')), may hold values from -64 to 64
- q_weight: bfloat16 [5120, 1024], P('dp', 'tensor'), may hold values from -0.69877124 to 0.69877124
- k_weight: bfloat16 [5120, 1024], P('dp'), may hold values from -0.69877124 to 0.69877124
- v_weight: bfloat16 [5120, 1024], P('dp'), may hold values from -0.078125 to 0.078125
- q_gain: float32 [1024], P('tensor'), may hold values from 0.1 to 1.9
- k_gain: float32 [1024], replicated, may hold values from 0.1 to 1.9
- o_weight: bfloat16 [1024, 5120], P('tensor', 'dp'), may hold values from -0.1875 to 0.1875
- post_gain: float32 [5120], replicated, may hold values from 0.1 to 1.9
Outputs:
- layer_out: bfloat16 [8192, 5120], P(('dp', 'tensor'))
The draws below stay inside these ranges and needn't reach their ends.
All inputs are finite; a program needn't handle non-finite values.
Results may differ from the reference program's by a relative error of at most 0.012.
Values may be sent and summed in bfloat16 or wider, within the bound.
No kernel may reach another device: no remote copies, remote signals or barrier semaphores. Data moves between devices by JAX's collectives and lax.ppermute only.
A program may use at most 128 MiB of HBM per device.

```python
import jax
import jax.numpy as jnp
from jax import lax

D = 5120
HD = 128
KV_HEADS = 8
HEADS_DEV = 2
SEQ = 1024
HEADS = 8
TOKENS = 8192
N_DP = 8


def clipped(key, shape):
    return jnp.clip(jax.random.normal(key, shape, jnp.float32), -6.0, 6.0)


def head_scales(key, count):
    ramp = jnp.exp(0.5 * jnp.log(3.0) * jnp.arange(count, dtype=jnp.float32) / (count - 1))
    return ramp * jax.random.uniform(key, (count,), jnp.float32, 0.7, 1.3)


def draw_hidden_in(key, part):
    base = clipped(jax.random.fold_in(key, 1), (TOKENS, D))
    return base.astype(jnp.bfloat16)


def draw_k_weight(key, part):
    base = clipped(jax.random.fold_in(key, 3), (D, KV_HEADS * HD)) * D ** (-0.5)
    return base.astype(jnp.bfloat16)


def draw_q_weight(key, part):
    base = clipped(jax.random.fold_in(key, 4), (D, HEADS, HD)) * D ** (-0.5)
    base = base * head_scales(jax.random.fold_in(key, 6), HEADS)[None, :, None]
    base = base.reshape(D, HEADS * HD)
    return base.astype(jnp.bfloat16)


def level_of(stream_key, dims, cuts, low, high):
    def one(position, parts):
        heights = jax.random.uniform(jax.random.fold_in(jax.random.fold_in(stream_key, 6), position), (parts,), jnp.float32, low / len(cuts), high / len(cuts))
        return jnp.repeat(jnp.exp(heights), dims[position] // parts).reshape((-1,) + (1,) * (len(dims) - position - 1))

    loudness = one(*cuts[0])
    for cut in cuts[1:]:
        loudness = loudness * one(*cut)
    return loudness


def normal_values(rng, dims, deviation, limit, pieces=(), kind=jnp.bfloat16):
    entries = deviation * jax.random.normal(rng, dims, jnp.float32)
    if pieces:
        entries = entries * level_of(rng, dims, pieces, -0.22, 0.18)
    return jnp.clip(entries, -limit, limit).astype(kind)


def setup_inputs(seed: int = 0) -> dict:
    keys = jax.random.split(jax.random.key(seed), 9)
    hidden_in = draw_hidden_in(jax.random.fold_in(keys[8], 71), 0)
    q_weight = draw_q_weight(jax.random.fold_in(keys[8], 71), 0)
    k_weight = draw_k_weight(jax.random.fold_in(keys[8], 71), 0)
    v_weight = normal_values(keys[3], (D, KV_HEADS * HD), D ** -0.5, 0.078125, ((0, 8),))
    q_gain = jnp.clip(1.0 + 0.18 * jax.random.normal(keys[4], (HEADS * HD,), jnp.float32), 0.1, 1.9)
    k_gain = jnp.clip(1.0 + 0.18 * jax.random.normal(keys[5], (KV_HEADS * HD,), jnp.float32), 0.1, 1.9)
    o_weight = normal_values(keys[6], (HEADS * HD, D), (HEADS * HD) ** -0.5, 0.1875, ((0, 4), (1, 8)))
    post_gain = jnp.clip(1.0 + 0.18 * jax.random.normal(keys[7], (D,), jnp.float32), 0.1, 1.9)
    return dict(hidden_in=hidden_in, q_weight=q_weight, k_weight=k_weight, v_weight=v_weight, q_gain=q_gain, k_gain=k_gain, o_weight=o_weight, post_gain=post_gain)


epsilon = 1e-06

def rms_scale(block, gain, width):
    mean_square = lax.optimization_barrier(jnp.sum(block * block, axis=1, keepdims=True)) / width
    return block * lax.rsqrt(mean_square + epsilon) * gain

def one_sequence(tokens, q_weight, k_weight, v_weight, q_gain, k_gain, o_weight, post_gain):
    queries = jnp.dot(tokens, q_weight, preferred_element_type=jnp.float32)
    key_rows = jnp.dot(tokens, k_weight, preferred_element_type=jnp.float32)
    value_rows = jnp.dot(tokens, v_weight, preferred_element_type=jnp.float32).astype(jnp.bfloat16)
    q_normed = rms_scale(queries, q_gain, HEADS * HD).astype(jnp.bfloat16)
    k_normed = rms_scale(key_rows, k_gain, KV_HEADS * HD).astype(jnp.bfloat16)
    group_size = HEADS // KV_HEADS
    q_heads = q_normed.astype(jnp.float32).reshape(SEQ, HEADS, HD)
    k_heads = jnp.repeat(k_normed.astype(jnp.float32).reshape(SEQ, KV_HEADS, HD), group_size, axis=1)
    v_heads = jnp.repeat(value_rows.astype(jnp.float32).reshape(SEQ, KV_HEADS, HD), group_size, axis=1)
    scores = jnp.einsum('qhd,khd->hqk', q_heads, k_heads) * HD ** (-0.5)
    rows_idx = lax.broadcasted_iota(jnp.int32, (SEQ, SEQ), 0)
    cols_idx = lax.broadcasted_iota(jnp.int32, (SEQ, SEQ), 1)
    scores = jnp.where((cols_idx <= rows_idx)[None], scores, -1e+30)
    row_max = lax.optimization_barrier(jnp.max(scores, axis=-1, keepdims=True))
    expo = jnp.exp(scores - row_max)
    soft_weights = (expo / lax.optimization_barrier(jnp.sum(expo, axis=-1, keepdims=True))).astype(jnp.bfloat16)
    attended = jnp.einsum('hqk,khd->qhd', soft_weights.astype(jnp.float32), v_heads).astype(jnp.bfloat16)
    blocks = HEADS // HEADS_DEV
    attended_blocks = attended.reshape(SEQ, blocks, HEADS_DEV * HD).astype(jnp.float32)
    weight_blocks = o_weight.reshape(blocks, HEADS_DEV * HD, D).astype(jnp.float32)
    partials = jnp.einsum('snk,nkd->nsd', attended_blocks, weight_blocks)
    rounded = lax.optimization_barrier(partials.astype(jnp.bfloat16)).astype(jnp.float32)
    projected = lax.optimization_barrier(jnp.sum(rounded, axis=0))
    mean_square = lax.optimization_barrier(jnp.mean(projected * projected, axis=1, keepdims=True))
    result = tokens.astype(jnp.float32) + projected * lax.rsqrt(mean_square + epsilon) * post_gain
    return result.astype(jnp.bfloat16)

def reference(hidden_in, q_weight, k_weight, v_weight, q_gain, k_gain, o_weight, post_gain):
    sequences = hidden_in.reshape(N_DP, SEQ, D)

    def apply_layer(tokens):
        return one_sequence(tokens, q_weight, k_weight, v_weight, q_gain, k_gain, o_weight, post_gain)
    outputs = lax.map(apply_layer, sequences)
    return outputs.reshape(TOKENS, D)
```

```python
import jax
import jax.numpy as jnp
from jax import lax
from jax.sharding import PartitionSpec as P

HD = 128
KV_HEADS = 8


epsilon = 1e-06


def after(value, *others):
    return lax.optimization_barrier((value,) + others)[0]


def attend(queries, key_rows, value_rows, q_total, k_total, q_gain, k_gain_part, position, sizes):
    heads_dev, kv_count, group_size, heads_all = sizes
    seq_len = queries.shape[0]
    q_normed = (queries * lax.rsqrt(q_total / (heads_all * HD) + epsilon)[:, None] * q_gain).astype(
        jnp.bfloat16
    )
    k_normed = (
        key_rows * lax.rsqrt(k_total / (KV_HEADS * HD) + epsilon)[:, None] * k_gain_part
    ).astype(jnp.bfloat16)
    value_cast = value_rows.astype(jnp.bfloat16)
    q_heads = q_normed.reshape(seq_len, heads_dev, HD)
    k_three = k_normed.reshape(seq_len, kv_count, HD)
    v_three = value_cast.reshape(seq_len, kv_count, HD)
    if heads_dev >= group_size:
        k_heads = jnp.repeat(k_three, group_size, axis=1)
        v_heads = jnp.repeat(v_three, group_size, axis=1)
    else:
        k_heads = jnp.broadcast_to(k_three, (seq_len, heads_dev, HD))
        v_heads = jnp.broadcast_to(v_three, (seq_len, heads_dev, HD))
    scores = jnp.einsum(
        "qhd,khd->hqk", q_heads, k_heads, preferred_element_type=jnp.float32
    ) * HD ** (-0.5)
    scores = jnp.where((position[None, :] <= position[:, None])[None], scores, -1e30)
    row_max = jnp.max(scores, axis=-1, keepdims=True)
    expo = jnp.exp(scores - row_max)
    soft_weights = (expo / jnp.sum(expo, axis=-1, keepdims=True)).astype(jnp.bfloat16)
    attended = jnp.einsum("hqk,khd->qhd", soft_weights, v_heads, preferred_element_type=jnp.float32)
    return attended.astype(jnp.bfloat16).reshape(seq_len, heads_dev * HD)


def finish(hidden_in, summed, post_gain):
    mean_square = jnp.mean(summed * summed, axis=1, keepdims=True)
    result = hidden_in.astype(jnp.float32) + summed * lax.rsqrt(mean_square + epsilon) * post_gain
    return result.astype(jnp.bfloat16)


def pair_swap(value, bit):
    return lax.ppermute(value, "tensor", [(i, i ^ bit) for i in range(lax.axis_size("tensor"))])


def core_swap(value, sources=None):
    dp_size = lax.axis_size("dp")
    sources = range(dp_size) if sources is None else sources
    return lax.ppermute(value, "dp", [(i, i ^ 1) for i in sources])


def z_flows(shard):
    planes = lax.axis_size("dp") // 2
    right, left = [shard], [shard]
    for step in range(1, planes):
        right.append(
            lax.ppermute(
                right[-1],
                "dp",
                [(2 * z + c, 2 * z + 2 + c) for z in range(step - 1, planes - 1) for c in (0, 1)],
            )
        )
        left.append(
            lax.ppermute(
                left[-1],
                "dp",
                [(2 * z + c, 2 * z - 2 + c) for z in range(1, planes - step + 1) for c in (0, 1)],
            )
        )
    return right, left


def z_merge(right, left, z):
    planes = len(right)
    return [right[0]] + [jnp.where(z >= r, right[r], left[planes - r]) for r in range(1, planes)]


def core_flows(right, left):
    planes = len(right)
    own = core_swap(right[0])
    right_other, left_other = [own], [own]
    for s in range(1, planes):
        right_other.append(
            core_swap(right[s], [2 * z + c for z in range(s, planes) for c in (0, 1)])
        )
        left_other.append(
            core_swap(left[s], [2 * z + c for z in range(0, planes - s) for c in (0, 1)])
        )
    return right_other, left_other


def exchange(a, b):
    xa, yb = pair_swap(a, 1), pair_swap(b, 2)
    xb, ya = pair_swap(b, 1), pair_swap(a, 2)
    da, db = pair_swap(xa, 2), pair_swap(yb, 1)
    return [(a, b), (xa, xb), (ya, yb), (da, db)]


def local(hidden_in, q_weight, k_weight, v_weight, q_gain, k_gain, o_weight, post_gain):
    heads_dev = q_weight.shape[1] // HD
    tensor_size = lax.axis_size("tensor")
    heads_all = heads_dev * tensor_size
    group_size = heads_all // KV_HEADS
    kv_count = max(1, heads_dev // group_size)
    t = lax.axis_index("tensor")
    kv_first = t * heads_dev // group_size
    k_share = min(1.0, heads_dev / group_size)
    q_width = heads_dev * HD
    kv_width = kv_count * HD
    k_cols = lax.dynamic_slice_in_dim(k_weight, kv_first * HD, kv_width, 1)
    v_cols = lax.dynamic_slice_in_dim(v_weight, kv_first * HD, kv_width, 1)
    k_gain_part = lax.dynamic_slice_in_dim(k_gain, kv_first * HD, kv_width, 0)
    sizes = (heads_dev, kv_count, group_size, heads_all)
    rows, width = hidden_in.shape
    seq_len = rows * tensor_size

    if tensor_size != 4:
        all_tokens = lax.all_gather(hidden_in, "tensor", axis=0, tiled=True)
        queries, key_rows, value_rows = (
            jnp.dot(
                all_tokens,
                lax.all_gather(w, "dp", axis=0, tiled=True),
                preferred_element_type=jnp.float32,
            )
            for w in (q_weight, k_cols, v_cols)
        )
        q_total = lax.psum(jnp.sum(queries * queries, axis=1), "tensor")
        k_total = lax.psum(jnp.sum(key_rows * key_rows, axis=1) * k_share, "tensor")
        attended = attend(
            queries, key_rows, value_rows, q_total, k_total, q_gain, k_gain_part,
            jnp.arange(seq_len), sizes,
        )
        partial_value = jnp.dot(
            attended,
            lax.all_gather(o_weight, "dp", axis=1, tiled=True),
            preferred_element_type=jnp.float32,
        )
        summed = lax.psum_scatter(
            partial_value.astype(jnp.bfloat16), "tensor", scatter_dimension=0, tiled=True
        ).astype(jnp.float32)
        return finish(hidden_in, summed, post_gain)

    dp_size = lax.axis_size("dp")
    planes = dp_size // 2
    z = lax.axis_index("dp") // 2
    c = lax.axis_index("dp") % 2

    half = width // 2
    tokens = exchange(hidden_in[:, :half], hidden_in[:, half:])

    shard = jnp.concatenate([q_weight, k_cols, v_cols], axis=1)
    right, left = z_flows(shard)
    right_other, left_other = core_flows(right, left)
    mine = z_merge(right, left, z)
    others = z_merge(right_other, left_other, z)
    block = shard.shape[0]
    weight = jnp.zeros((dp_size * block, shard.shape[1]), shard.dtype)
    for r in range(planes):
        base = ((z - r) % planes) * 2
        weight = lax.dynamic_update_slice_in_dim(weight, mine[r], (base + c) * block, 0)
        weight = lax.dynamic_update_slice_in_dim(weight, others[r], (base + 1 - c) * block, 0)

    o_shard = after(o_weight.T, right[planes - 2], left[planes - 2])
    o_mine = z_merge(*z_flows(o_shard), z)
    cut = planes // 2
    o_parts = exchange(jnp.concatenate(o_mine[:cut], 0), jnp.concatenate(o_mine[cut:], 0))
    o_parts_other = [tuple(core_swap(v) for v in pair) for pair in o_parts]

    projected = [
        jnp.dot(a, weight[:half], preferred_element_type=jnp.float32)
        + jnp.dot(b, weight[half:], preferred_element_type=jnp.float32)
        for a, b in tokens
    ]
    rows_all = jnp.concatenate(projected, axis=0)
    queries = rows_all[:, :q_width]
    key_rows = rows_all[:, q_width : q_width + kv_width]
    value_rows = rows_all[:, q_width + kv_width :]
    sums = jnp.stack(
        [jnp.sum(queries * queries, axis=1), jnp.sum(key_rows * key_rows, axis=1) * k_share]
    ).reshape(2, tensor_size, rows)
    total = sums
    for bit in range(1, tensor_size):
        theirs = pair_swap(sums, bit)
        total = total + theirs[:, jnp.array([i ^ bit for i in range(tensor_size)])]
    total = total.reshape(2, seq_len)
    position = jnp.concatenate([(t ^ i) * rows + jnp.arange(rows) for i in range(tensor_size)])
    attended = attend(
        queries, key_rows, value_rows, total[0], total[1], q_gain, k_gain_part, position, sizes
    )
    heads_of = [attended[:rows]] + [
        pair_swap(attended[i * rows : (i + 1) * rows], i) for i in range(1, tensor_size)
    ]

    def project(parts, index):
        return sum(
            lax.dot_general(
                heads_of[i], parts[i][index], (((1,), (1,)), ((), ())),
                preferred_element_type=jnp.float32,
            )
            for i in range(tensor_size)
        )

    relative = jnp.stack(
        [
            piece
            for parts in (o_parts, o_parts_other)
            for index in (0, 1)
            for piece in jnp.split(project(parts, index), cut if index == 0 else planes - cut, 1)
        ]
    )
    summed = jnp.concatenate(
        [
            lax.dynamic_index_in_dim(
                relative, ((j % 2) ^ c) * planes + (z - j // 2) % planes, 0, keepdims=False
            )
            for j in range(dp_size)
        ],
        axis=1,
    )
    return finish(hidden_in, summed, post_gain)


def solution(mesh):
    in_specs = (
        P(("dp", "tensor"), None),
        P("dp", "tensor"),
        P("dp", None),
        P("dp", None),
        P("tensor"),
        P(),
        P("tensor", "dp"),
        P(),
    )
    out_specs = P(("dp", "tensor"), None)
    return jax.shard_map(local, mesh=mesh, in_specs=in_specs, out_specs=out_specs, check_vma=False)
```

```python
import jax
import jax.numpy as jnp
from jax import lax
from jax.experimental import pallas as pl
from jax.experimental.pallas import tpu as pltpu
from jax.sharding import PartitionSpec as P

HD = 128
KV_HEADS = 8


epsilon = 1e-06


def after(value, *others):
    return lax.optimization_barrier((value,) + others)[0]


def attend(queries, key_rows, value_rows, q_total, k_total, q_gain, k_gain_part, position, sizes):
    heads_dev, kv_count, group_size, heads_all = sizes
    seq_len = queries.shape[0]
    q_normed = (queries * lax.rsqrt(q_total / (heads_all * HD) + epsilon)[:, None] * q_gain).astype(
        jnp.bfloat16
    )
    k_normed = (
        key_rows * lax.rsqrt(k_total / (KV_HEADS * HD) + epsilon)[:, None] * k_gain_part
    ).astype(jnp.bfloat16)
    value_cast = value_rows.astype(jnp.bfloat16)
    q_heads = q_normed.reshape(seq_len, heads_dev, HD)
    k_three = k_normed.reshape(seq_len, kv_count, HD)
    v_three = value_cast.reshape(seq_len, kv_count, HD)
    if heads_dev >= group_size:
        k_heads = jnp.repeat(k_three, group_size, axis=1)
        v_heads = jnp.repeat(v_three, group_size, axis=1)
    else:
        k_heads = jnp.broadcast_to(k_three, (seq_len, heads_dev, HD))
        v_heads = jnp.broadcast_to(v_three, (seq_len, heads_dev, HD))
    scores = jnp.einsum(
        "qhd,khd->hqk", q_heads, k_heads, preferred_element_type=jnp.float32
    ) * HD ** (-0.5)
    scores = jnp.where((position[None, :] <= position[:, None])[None], scores, -1e30)
    row_max = jnp.max(scores, axis=-1, keepdims=True)
    expo = jnp.exp(scores - row_max)
    soft_weights = (expo / jnp.sum(expo, axis=-1, keepdims=True)).astype(jnp.bfloat16)
    attended = jnp.einsum("hqk,khd->qhd", soft_weights, v_heads, preferred_element_type=jnp.float32)
    return attended.astype(jnp.bfloat16).reshape(seq_len, heads_dev * HD)


def finish(hidden_in, summed, post_gain):
    mean_square = jnp.mean(summed * summed, axis=1, keepdims=True)
    result = hidden_in.astype(jnp.float32) + summed * lax.rsqrt(mean_square + epsilon) * post_gain
    return result.astype(jnp.bfloat16)


def pair_swap(value, bit):
    return lax.ppermute(value, "tensor", [(i, i ^ bit) for i in range(lax.axis_size("tensor"))])


def core_swap(value, sources=None):
    dp_size = lax.axis_size("dp")
    sources = range(dp_size) if sources is None else sources
    return lax.ppermute(value, "dp", [(i, i ^ 1) for i in sources])


def z_flows(shard):
    planes = lax.axis_size("dp") // 2
    right, left = [shard], [shard]
    for step in range(1, planes):
        right.append(
            lax.ppermute(
                right[-1],
                "dp",
                [(2 * z + c, 2 * z + 2 + c) for z in range(step - 1, planes - 1) for c in (0, 1)],
            )
        )
        left.append(
            lax.ppermute(
                left[-1],
                "dp",
                [(2 * z + c, 2 * z - 2 + c) for z in range(1, planes - step + 1) for c in (0, 1)],
            )
        )
    return right, left


def z_merge(right, left, z):
    planes = len(right)
    return [right[0]] + [jnp.where(z >= r, right[r], left[planes - r]) for r in range(1, planes)]


def core_flows(right, left):
    planes = len(right)
    own = core_swap(right[0])
    right_other, left_other = [own], [own]
    for s in range(1, planes):
        right_other.append(
            core_swap(right[s], [2 * z + c for z in range(s, planes) for c in (0, 1)])
        )
        left_other.append(
            core_swap(left[s], [2 * z + c for z in range(0, planes - s) for c in (0, 1)])
        )
    return right_other, left_other


def exchange(value, axis):
    half = value.shape[axis] // 2
    x, y = pair_swap(value, 1), pair_swap(value, 2)
    da = pair_swap(lax.slice_in_dim(x, 0, half, axis=axis), 2)
    db = pair_swap(lax.slice_in_dim(y, half, None, axis=axis), 1)
    return x, y, da, db


def assemble(mine, others, z, c, gate):
    planes = len(mine)
    block = mine[0].shape[0]
    zero = after(jnp.zeros((), mine[0].dtype), gate)
    weight = jnp.broadcast_to(zero, (2 * planes * block, mine[0].shape[1]))
    for r in range(planes):
        base = ((z - r) % planes) * 2
        weight = lax.dynamic_update_slice_in_dim(weight, mine[r], (base + c) * block, 0)
        weight = lax.dynamic_update_slice_in_dim(weight, others[r], (base + 1 - c) * block, 0)
    return weight


def project_kernel(planes, place, *refs):
    parts, (hidden, gain, out, proj) = refs[:14], refs[14:]
    heads_of = parts[:4]
    j = pl.program_id(0)
    base = ((place[0] - j + planes) % planes) * 2
    for side in range(2):
        pieces = parts[4 + 5 * side : 9 + 5 * side]
        diagonal = jnp.where(j < planes // 2, pieces[3][...], pieces[4][...])
        total = None
        for i in range(4):
            right = pieces[i][...] if i < 3 else diagonal
            term = lax.dot_general(
                heads_of[i][...], right, (((1,), (1,)), ((), ())),
                preferred_element_type=jnp.float32,
            )
            total = term if total is None else total + term
        proj[base + (place[1] if side == 0 else 1 - place[1])] = total

    @pl.when(j == planes - 1)
    def _():
        block = proj.shape[2]
        square = None
        for n in range(2 * planes):
            value = proj[n]
            term = jnp.sum(value * value, axis=1, keepdims=True)
            square = term if square is None else square + term
        scale = lax.rsqrt(square / (2 * planes * block) + epsilon)
        for n in range(2 * planes):
            cols = slice(n * block, (n + 1) * block)
            value = hidden[:, cols].astype(jnp.float32) + proj[n] * scale * gain[:, cols]
            out[:, cols] = value.astype(out.dtype)


def project(heads_of, own, other, hidden_in, post_gain, z, c, planes):
    rows, width = hidden_in.shape
    depth = heads_of[0].shape[1]
    block = width // (2 * planes)
    cut = planes // 2
    whole = lambda j, place: (0, 0)
    each = pl.BlockSpec((block, depth), lambda j, place: (j, 0))
    low = pl.BlockSpec((block, depth), lambda j, place: (jnp.minimum(j, cut - 1), 0))
    high = pl.BlockSpec((block, depth), lambda j, place: (jnp.maximum(j - cut, 0), 0))
    spec = pltpu.PrefetchScalarGridSpec(
        num_scalar_prefetch=1,
        grid=(planes,),
        in_specs=[pl.BlockSpec((rows, depth), whole)] * 4
        + [each, each, each, low, high] * 2
        + [pl.BlockSpec((rows, width), whole), pl.BlockSpec((1, width), whole)],
        out_specs=pl.BlockSpec((rows, width), whole),
        scratch_shapes=[pltpu.VMEM((2 * planes, rows, block), jnp.float32)],
    )
    return pl.pallas_call(
        lambda *refs: project_kernel(planes, *refs),
        grid_spec=spec,
        out_shape=jax.ShapeDtypeStruct((rows, width), hidden_in.dtype),
        name="project",
    )(
        jnp.stack([z, c]).astype(jnp.int32), *heads_of, *own, *other, hidden_in, post_gain[None, :]
    )


def local(hidden_in, q_weight, k_weight, v_weight, q_gain, k_gain, o_weight, post_gain):
    heads_dev = q_weight.shape[1] // HD
    tensor_size = lax.axis_size("tensor")
    heads_all = heads_dev * tensor_size
    group_size = heads_all // KV_HEADS
    kv_count = max(1, heads_dev // group_size)
    t = lax.axis_index("tensor")
    kv_first = t * heads_dev // group_size
    k_share = min(1.0, heads_dev / group_size)
    q_width = heads_dev * HD
    kv_width = kv_count * HD
    k_cols = lax.dynamic_slice_in_dim(k_weight, kv_first * HD, kv_width, 1)
    v_cols = lax.dynamic_slice_in_dim(v_weight, kv_first * HD, kv_width, 1)
    k_gain_part = lax.dynamic_slice_in_dim(k_gain, kv_first * HD, kv_width, 0)
    sizes = (heads_dev, kv_count, group_size, heads_all)
    rows, width = hidden_in.shape
    seq_len = rows * tensor_size

    if tensor_size != 4:
        all_tokens = lax.all_gather(hidden_in, "tensor", axis=0, tiled=True)
        queries, key_rows, value_rows = (
            jnp.dot(
                all_tokens,
                lax.all_gather(w, "dp", axis=0, tiled=True),
                preferred_element_type=jnp.float32,
            )
            for w in (q_weight, k_cols, v_cols)
        )
        q_total = lax.psum(jnp.sum(queries * queries, axis=1), "tensor")
        k_total = lax.psum(jnp.sum(key_rows * key_rows, axis=1) * k_share, "tensor")
        attended = attend(
            queries, key_rows, value_rows, q_total, k_total, q_gain, k_gain_part,
            jnp.arange(seq_len), sizes,
        )
        partial_value = jnp.dot(
            attended,
            lax.all_gather(o_weight, "dp", axis=1, tiled=True),
            preferred_element_type=jnp.float32,
        )
        summed = lax.psum_scatter(
            partial_value.astype(jnp.bfloat16), "tensor", scatter_dimension=0, tiled=True
        ).astype(jnp.float32)
        return finish(hidden_in, summed, post_gain)

    dp_size = lax.axis_size("dp")
    planes = dp_size // 2
    z = lax.axis_index("dp") // 2
    c = lax.axis_index("dp") % 2

    half = width // 2
    x_tokens, y_tokens, da_tokens, db_tokens = exchange(hidden_in, 1)

    qk_shard = jnp.concatenate([q_weight, k_cols], axis=1)
    qk_flows = z_flows(qk_shard)
    vo_shard = after(
        jnp.concatenate([v_cols, o_weight.T], axis=1), qk_flows[0][planes - 2], qk_flows[1][planes - 2]
    )
    vo_flows = z_flows(vo_shard)
    qk_mine, qk_others = z_merge(*qk_flows, z), z_merge(*core_flows(*qk_flows), z)
    vo_mine, vo_others = z_merge(*vo_flows, z), z_merge(*core_flows(*vo_flows), z)
    qk_full = assemble(qk_mine, qk_others, z, c, qk_flows[0][1][0, 0])

    def times(weight):
        return jnp.concatenate(
            [jnp.dot(a, weight, preferred_element_type=jnp.float32) for a in (hidden_in, x_tokens, y_tokens)]
            + [
                jnp.dot(da_tokens, weight[:half], preferred_element_type=jnp.float32)
                + jnp.dot(db_tokens, weight[half:], preferred_element_type=jnp.float32)
            ],
            axis=0,
        )

    qk_rows = times(qk_full)
    queries, key_rows = qk_rows[:, :q_width], qk_rows[:, q_width:]
    sums = jnp.stack(
        [jnp.sum(queries * queries, axis=1), jnp.sum(key_rows * key_rows, axis=1) * k_share]
    )
    total = sums
    for bit in range(1, tensor_size):
        moved = [sums[:, (i ^ bit) * rows : ((i ^ bit) + 1) * rows] for i in range(tensor_size)]
        total = total + pair_swap(jnp.concatenate(moved, axis=1), bit)

    v_full = assemble(
        [m[:, :kv_width] for m in vo_mine], [m[:, :kv_width] for m in vo_others], z, c,
        vo_flows[0][1][0, 0],
    )
    value_rows = times(v_full)

    o_own = jnp.concatenate([m[:, kv_width:] for m in vo_mine], axis=0)
    o_other = jnp.concatenate([m[:, kv_width:] for m in vo_others], axis=0)
    o_parts = exchange(o_own, 0)
    o_parts_other = tuple(core_swap(v) for v in o_parts)

    position = jnp.concatenate([(t ^ i) * rows + jnp.arange(rows) for i in range(tensor_size)])
    attended = attend(
        queries, key_rows, value_rows, total[0], total[1], q_gain, k_gain_part, position, sizes
    )
    heads_of = [attended[:rows]] + [
        pair_swap(attended[i * rows : (i + 1) * rows], i) for i in range(1, tensor_size)
    ]
    return project(
        heads_of, (o_own,) + o_parts, (o_other,) + o_parts_other, hidden_in, post_gain, z, c, planes
    )


def solution(mesh):
    in_specs = (
        P(("dp", "tensor"), None),
        P("dp", "tensor"),
        P("dp", None),
        P("dp", None),
        P("tensor"),
        P(),
        P("tensor", "dp"),
        P(),
    )
    out_specs = P(("dp", "tensor"), None)
    return jax.shard_map(local, mesh=mesh, in_specs=in_specs, out_specs=out_specs, check_vma=False)
```

```python
import jax
import jax.numpy as jnp
from jax import lax
from jax.experimental import pallas as pl
from jax.experimental.pallas import tpu as pltpu
from jax.sharding import PartitionSpec as P

HD = 128
KV_HEADS = 8


epsilon = 1e-06


def after(value, *others):
    return lax.optimization_barrier((value,) + others)[0]


def attend(queries, key_rows, value_rows, q_total, k_total, q_gain, k_gain_part, position, sizes):
    heads_dev, kv_count, group_size, heads_all = sizes
    seq_len = queries.shape[0]
    q_normed = (queries * lax.rsqrt(q_total / (heads_all * HD) + epsilon)[:, None] * q_gain).astype(
        jnp.bfloat16
    )
    k_normed = (
        key_rows * lax.rsqrt(k_total / (KV_HEADS * HD) + epsilon)[:, None] * k_gain_part
    ).astype(jnp.bfloat16)
    value_cast = value_rows.astype(jnp.bfloat16)
    q_heads = q_normed.reshape(seq_len, heads_dev, HD)
    k_three = k_normed.reshape(seq_len, kv_count, HD)
    v_three = value_cast.reshape(seq_len, kv_count, HD)
    if heads_dev >= group_size:
        k_heads = jnp.repeat(k_three, group_size, axis=1)
        v_heads = jnp.repeat(v_three, group_size, axis=1)
    else:
        k_heads = jnp.broadcast_to(k_three, (seq_len, heads_dev, HD))
        v_heads = jnp.broadcast_to(v_three, (seq_len, heads_dev, HD))
    scores = jnp.einsum(
        "qhd,khd->hqk", q_heads, k_heads, preferred_element_type=jnp.float32
    ) * HD ** (-0.5)
    scores = jnp.where((position[None, :] <= position[:, None])[None], scores, -1e30)
    row_max = jnp.max(scores, axis=-1, keepdims=True)
    expo = jnp.exp(scores - row_max)
    soft_weights = (expo / jnp.sum(expo, axis=-1, keepdims=True)).astype(jnp.bfloat16)
    attended = jnp.einsum("hqk,khd->hqd", soft_weights, v_heads, preferred_element_type=jnp.float32)
    return attended.astype(jnp.bfloat16)


def finish(hidden_in, summed, post_gain):
    mean_square = jnp.mean(summed * summed, axis=1, keepdims=True)
    result = hidden_in.astype(jnp.float32) + summed * lax.rsqrt(mean_square + epsilon) * post_gain
    return result.astype(jnp.bfloat16)


def pair_swap(value, bit):
    return lax.ppermute(value, "tensor", [(i, i ^ bit) for i in range(lax.axis_size("tensor"))])


def core_swap(value, sources=None):
    dp_size = lax.axis_size("dp")
    sources = range(dp_size) if sources is None else sources
    return lax.ppermute(value, "dp", [(i, i ^ 1) for i in sources])


def z_flows(shard):
    planes = lax.axis_size("dp") // 2
    right, left = [shard], [shard]
    for step in range(1, planes):
        right.append(
            lax.ppermute(
                right[-1],
                "dp",
                [(2 * z + c, 2 * z + 2 + c) for z in range(step - 1, planes - 1) for c in (0, 1)],
            )
        )
        left.append(
            lax.ppermute(
                left[-1],
                "dp",
                [(2 * z + c, 2 * z - 2 + c) for z in range(1, planes - step + 1) for c in (0, 1)],
            )
        )
    return right, left


def z_merge(right, left, z):
    planes = len(right)
    return [right[0]] + [jnp.where(z >= r, right[r], left[planes - r]) for r in range(1, planes)]


def core_flows(right, left, *gates):
    planes = len(right)
    if gates:
        right = right[:-1] + [after(right[-1], *gates)]
        left = left[:-1] + [after(left[-1], *gates)]
    own = core_swap(right[0])
    right_other, left_other = [own], [own]
    for s in range(1, planes):
        right_other.append(
            core_swap(right[s], [2 * z + c for z in range(s, planes) for c in (0, 1)])
        )
        left_other.append(
            core_swap(left[s], [2 * z + c for z in range(0, planes - s) for c in (0, 1)])
        )
    return right_other, left_other


def exchange(value, axis):
    half = value.shape[axis] // 2
    x, y = pair_swap(value, 1), pair_swap(value, 2)
    da = pair_swap(lax.slice_in_dim(x, 0, half, axis=axis), 2)
    db = pair_swap(lax.slice_in_dim(y, half, None, axis=axis), 1)
    return x, y, da, db


def assemble(mine, others, z, c, gate):
    planes = len(mine)
    block = mine[0].shape[0]
    zero = jnp.where(z < 0, gate, 0)
    weight = jnp.broadcast_to(zero, (2 * planes * block, mine[0].shape[1]))
    for r in range(planes):
        base = ((z - r) % planes) * 2
        weight = lax.dynamic_update_slice_in_dim(weight, mine[r], (base + c) * block, 0)
        weight = lax.dynamic_update_slice_in_dim(weight, others[r], (base + 1 - c) * block, 0)
    return weight


def project_kernel(planes, place, *refs):
    parts, (hidden, gain, out, proj) = refs[:14], refs[14:]
    heads_of = [
        jnp.concatenate([part[h] for h in range(part.shape[0])], axis=1) for part in parts[:4]
    ]
    j = pl.program_id(0)
    base = ((place[0] - j + planes) % planes) * 2
    for side in range(2):
        pieces = parts[4 + 5 * side : 9 + 5 * side]
        diagonal = jnp.where(j < planes // 2, pieces[3][...], pieces[4][...])
        total = None
        for i in range(4):
            right = pieces[i][...] if i < 3 else diagonal
            term = lax.dot_general(
                heads_of[i], right, (((1,), (1,)), ((), ())),
                preferred_element_type=jnp.float32,
            )
            total = term if total is None else total + term
        proj[base + (place[1] if side == 0 else 1 - place[1])] = total

    @pl.when(j == planes - 1)
    def _():
        block = proj.shape[2]
        square = None
        for n in range(2 * planes):
            value = proj[n]
            term = jnp.sum(value * value, axis=1, keepdims=True)
            square = term if square is None else square + term
        scale = lax.rsqrt(square / (2 * planes * block) + epsilon)
        for n in range(2 * planes):
            cols = slice(n * block, (n + 1) * block)
            value = hidden[:, cols].astype(jnp.float32) + proj[n] * scale * gain[:, cols]
            out[:, cols] = value.astype(out.dtype)


def project(heads_of, own, other, hidden_in, post_gain, z, c, planes):
    rows, width = hidden_in.shape
    depth = own[0].shape[1]
    block = width // (2 * planes)
    cut = planes // 2
    whole = lambda j, place: (0, 0)
    each = pl.BlockSpec((block, depth), lambda j, place: (j, 0))
    low = pl.BlockSpec((block, depth), lambda j, place: (jnp.minimum(j, cut - 1), 0))
    high = pl.BlockSpec((block, depth), lambda j, place: (jnp.maximum(j - cut, 0), 0))
    spec = pltpu.PrefetchScalarGridSpec(
        num_scalar_prefetch=1,
        grid=(planes,),
        in_specs=[pl.BlockSpec(heads_of[0].shape, lambda j, place: (0, 0, 0))] * 4
        + [each, each, each, low, high] * 2
        + [pl.BlockSpec((rows, width), whole), pl.BlockSpec((1, width), whole)],
        out_specs=pl.BlockSpec((rows, width), whole),
        scratch_shapes=[pltpu.VMEM((2 * planes, rows, block), jnp.float32)],
    )
    return pl.pallas_call(
        lambda *refs: project_kernel(planes, *refs),
        grid_spec=spec,
        out_shape=jax.ShapeDtypeStruct((rows, width), hidden_in.dtype),
        name="project",
    )(
        jnp.stack([z, c]).astype(jnp.int32), *heads_of, *own, *other, hidden_in, post_gain[None, :]
    )


def local(hidden_in, q_weight, k_weight, v_weight, q_gain, k_gain, o_weight, post_gain):
    heads_dev = q_weight.shape[1] // HD
    tensor_size = lax.axis_size("tensor")
    heads_all = heads_dev * tensor_size
    group_size = heads_all // KV_HEADS
    kv_count = max(1, heads_dev // group_size)
    t = lax.axis_index("tensor")
    kv_first = t * heads_dev // group_size
    k_share = min(1.0, heads_dev / group_size)
    q_width = heads_dev * HD
    kv_width = kv_count * HD
    k_cols = lax.dynamic_slice_in_dim(k_weight, kv_first * HD, kv_width, 1)
    v_cols = lax.dynamic_slice_in_dim(v_weight, kv_first * HD, kv_width, 1)
    k_gain_part = lax.dynamic_slice_in_dim(k_gain, kv_first * HD, kv_width, 0)
    sizes = (heads_dev, kv_count, group_size, heads_all)
    rows, width = hidden_in.shape
    seq_len = rows * tensor_size

    if tensor_size != 4:
        all_tokens = lax.all_gather(hidden_in, "tensor", axis=0, tiled=True)
        queries, key_rows, value_rows = (
            jnp.dot(
                all_tokens,
                lax.all_gather(w, "dp", axis=0, tiled=True),
                preferred_element_type=jnp.float32,
            )
            for w in (q_weight, k_cols, v_cols)
        )
        q_total = lax.psum(jnp.sum(queries * queries, axis=1), "tensor")
        k_total = lax.psum(jnp.sum(key_rows * key_rows, axis=1) * k_share, "tensor")
        attended = attend(
            queries, key_rows, value_rows, q_total, k_total, q_gain, k_gain_part,
            jnp.arange(seq_len), sizes,
        )
        partial_value = jnp.dot(
            attended.transpose(1, 0, 2).reshape(seq_len, q_width),
            lax.all_gather(o_weight, "dp", axis=1, tiled=True),
            preferred_element_type=jnp.float32,
        )
        summed = lax.psum_scatter(
            partial_value.astype(jnp.bfloat16), "tensor", scatter_dimension=0, tiled=True
        ).astype(jnp.float32)
        return finish(hidden_in, summed, post_gain)

    dp_size = lax.axis_size("dp")
    planes = dp_size // 2
    z = lax.axis_index("dp") // 2
    c = lax.axis_index("dp") % 2

    half = width // 2
    x_tokens, y_tokens, da_tokens, db_tokens = exchange(hidden_in, 1)

    qk_shard = jnp.concatenate([q_weight, k_cols], axis=1)
    qk_flows = z_flows(qk_shard)
    vo_shard = jnp.concatenate([v_cols, o_weight.T], axis=1)
    vo_flows = z_flows(vo_shard)
    qk_mine, qk_others = z_merge(*qk_flows, z), z_merge(
        *core_flows(*qk_flows, x_tokens, y_tokens), z
    )
    vo_mine, vo_others = z_merge(*vo_flows, z), z_merge(*core_flows(*vo_flows), z)
    qk_full = assemble(qk_mine, qk_others, z, c, qk_flows[0][1][0, 0])

    def times(weight):
        return jnp.concatenate(
            [jnp.dot(a, weight, preferred_element_type=jnp.float32) for a in (hidden_in, x_tokens, y_tokens)]
            + [
                jnp.dot(da_tokens, weight[:half], preferred_element_type=jnp.float32)
                + jnp.dot(db_tokens, weight[half:], preferred_element_type=jnp.float32)
            ],
            axis=0,
        )

    qk_rows = times(qk_full)
    queries, key_rows = qk_rows[:, :q_width], qk_rows[:, q_width:]
    sums = jnp.stack(
        [jnp.sum(queries * queries, axis=1), jnp.sum(key_rows * key_rows, axis=1) * k_share]
    )
    total = sums
    for bit in range(1, tensor_size):
        moved = [sums[:, (i ^ bit) * rows : ((i ^ bit) + 1) * rows] for i in range(tensor_size)]
        total = total + pair_swap(jnp.concatenate(moved, axis=1), bit)

    v_full = assemble(
        [m[:, :kv_width] for m in vo_mine], [m[:, :kv_width] for m in vo_others], z, c,
        vo_flows[0][1][0, 0],
    )
    value_rows = times(v_full)

    o_own = jnp.concatenate([m[:, kv_width:] for m in vo_mine], axis=0)
    o_other = jnp.concatenate([m[:, kv_width:] for m in vo_others], axis=0)
    o_parts = exchange(after(o_own, da_tokens, db_tokens), 0)
    o_parts_other = tuple(core_swap(v) for v in o_parts)

    position = jnp.concatenate([(t ^ i) * rows + jnp.arange(rows) for i in range(tensor_size)])
    attended = attend(
        queries, key_rows, value_rows, total[0], total[1], q_gain, k_gain_part, position, sizes
    )
    heads_of = [attended[:, :rows]] + [
        pair_swap(attended[:, i * rows : (i + 1) * rows], i) for i in range(1, tensor_size)
    ]
    return project(
        heads_of, (o_own,) + o_parts, (o_other,) + o_parts_other, hidden_in, post_gain, z, c, planes
    )


def solution(mesh):
    in_specs = (
        P(("dp", "tensor"), None),
        P("dp", "tensor"),
        P("dp", None),
        P("dp", None),
        P("tensor"),
        P(),
        P("tensor", "dp"),
        P(),
    )
    out_specs = P(("dp", "tensor"), None)
    return jax.shard_map(local, mesh=mesh, in_specs=in_specs, out_specs=out_specs, check_vma=False)
```
